128 devices in a mesh: band: 16 (over x, y), sub: 8 (over z, core).
Axes of the slice: x: 4, y: 4, z: 4, core: 2. Of those that a mesh axis runs over, the one named last changes fastest.
Arguments:
- gas_amounts: bfloat16 [1024, 64, 8, 128], P('band'), may hold values from 0.049804688 to 1
- layer_mass: bfloat16 [1024, 64, 128], P('band'), may hold values from 4 to 40
- column_state: bfloat16 [1024, 2, 128], P('band'), may hold values from 0.099609375 to 0.796875
- absorption: bfloat16 [112, 8], P('sub'), may hold values from 0.0019989014 to 0.5
- single_scatter: float32 [112], P('sub'), may hold values from 0.2 to 0.95
- solar_weight: float32 [112], P('sub'), may hold values from 0.002 to 0.1
- sunlit: int32 [1024], replicated, may hold values from 0 to 1, as said below
Outputs:
- heating: float32 [1024, 64, 128], P(('band', 'sub'))
- surface_down: float32 [1024, 128], P(('band', 'sub'))
The draws below stay inside these ranges and needn't reach their ends.
Inputs may be any that keep to these rules, and one draw needn't show every extreme that they name: Exactly 512 blocks are sunlit, and in every draw all 64 blocks of some band index are sunlit.
All inputs are finite; a program needn't handle non-finite values.
Results may differ from the reference program's by a relative error of at most 0.0003.
Values may be sent and summed in bfloat16 or wider, within the bound.
A program may use at most 192 MiB of HBM per device.

```python
import math
import jax
import jax.numpy as jnp
from jax import lax

LEVELS = 64
GPOINTS = 112
GASES = 8
BLOCK_COLS = 128
BLK_DEV = 64
BLOCKS = 1024


def draw_sunlit(key, part):
    base = jax.random.fold_in(key, 17)
    key_shift, key_noise, key_top = jax.random.split(base, 3)
    band_total = BLOCKS // BLK_DEV
    shifts = jax.random.randint(key_shift, (band_total,), 0, 4).astype(jnp.int32)
    chosen = jax.random.randint(key_top, (), 0, band_total).astype(jnp.int32)
    shifts = shifts + jnp.where(jnp.arange(band_total, dtype=jnp.int32) == chosen, 8, 0).astype(jnp.int32)
    noise = jax.random.randint(key_noise, (BLOCKS,), 0, 65536).astype(jnp.int32)
    scores = (jnp.repeat(shifts, BLK_DEV) * 65536 + noise) * BLOCKS + jnp.arange(BLOCKS, dtype=jnp.int32)
    _, picked = lax.top_k(scores, BLOCKS // 2)
    return jnp.zeros((BLOCKS,), jnp.int32).at[picked].set(1)


def block_scale(own_key, extent, pieces, smallest, largest):
    def one(position, blocks):
        draws = jax.random.uniform(jax.random.fold_in(jax.random.fold_in(own_key, 6), position), (blocks,), jnp.float32, smallest / len(pieces), largest / len(pieces))
        return jnp.repeat(jnp.exp(draws), extent[position] // blocks).reshape((-1,) + (1,) * (len(extent) - position - 1))

    factor_of = one(*pieces[0])
    for cut in pieces[1:]:
        factor_of = factor_of * one(*cut)
    return factor_of


def setup_inputs(seed: int = 0) -> dict:
    key_of = jax.random.split(jax.random.key(seed), 8)
    gas_amounts = jnp.clip(jnp.exp(math.log(1.0) - 2.9996462 * jax.random.uniform(key_of[0], (BLOCKS, LEVELS, GASES, BLOCK_COLS), jnp.float32) ** block_scale(key_of[0], (BLOCKS, LEVELS, GASES, BLOCK_COLS), ((0, 16),), -0.2, 0.2)), 0.049804688, 1.0).astype(jnp.bfloat16)
    layer_mass = jnp.clip(jnp.exp(math.log(40.0) - 2.3025851 * jax.random.uniform(key_of[1], (BLOCKS, LEVELS, BLOCK_COLS), jnp.float32) ** block_scale(key_of[1], (BLOCKS, LEVELS, BLOCK_COLS), ((0, 16),), -0.2, 0.2)), 4.0, 40.0).astype(jnp.bfloat16)
    column_state = jnp.clip(0.099609375 + 0.6972656 * jax.random.uniform(key_of[2], (BLOCKS, 2, BLOCK_COLS), jnp.float32) ** block_scale(key_of[2], (BLOCKS, 2, BLOCK_COLS), ((0, 16),), -0.2, 0.2), 0.099609375, 0.796875).astype(jnp.bfloat16)
    absorption = jnp.clip(jnp.exp(math.log(0.5) - 5.5220104 * jax.random.uniform(key_of[3], (GPOINTS, GASES), jnp.float32) ** block_scale(key_of[3], (GPOINTS, GASES), ((0, 8),), -0.2, 0.2)), 0.0019989014, 0.5).astype(jnp.bfloat16)
    single_scatter = jnp.clip(0.2 + 0.75 * jax.random.uniform(key_of[4], (GPOINTS,), jnp.float32) ** block_scale(key_of[4], (GPOINTS,), ((0, 8),), -0.2, 0.2), 0.2, 0.95)
    solar_weight = jnp.clip(jnp.exp(math.log(0.1) - 3.912023 * jax.random.uniform(key_of[5], (GPOINTS,), jnp.float32) ** block_scale(key_of[5], (GPOINTS,), ((0, 8),), -0.2, 0.2)), 0.002, 0.1)
    sunlit = draw_sunlit(jax.random.fold_in(key_of[7], 71), 0)
    return dict(gas_amounts=gas_amounts, layer_mass=layer_mass, column_state=column_state, absorption=absorption, single_scatter=single_scatter, solar_weight=solar_weight, sunlit=sunlit)


def layer_solve(optical, heat_factor, cosine, ground, single_scatter, solar_weight):
    omega = single_scatter[:, None]
    passing = jnp.exp(-optical)
    reflected = 0.5 * omega * (1.0 - passing * passing)
    unscattered = jnp.exp(-optical / cosine[None, None, :])

    def upward(lower_albedo, layer_data):
        reflect_now, pass_now = layer_data
        denominator = 1.0 - reflect_now * lower_albedo
        upper_albedo = reflect_now + pass_now * pass_now * lower_albedo / denominator
        return upper_albedo, (upper_albedo, denominator)

    surface = jnp.broadcast_to(ground[None, :], optical.shape[1:])
    _, (stack_albedo, denominators) = lax.scan(upward, surface, (reflected, passing), reverse=True, unroll=8)

    def downward(state_now, layer_data):
        beam, diffuse = state_now
        albedo_now, pass_now, direct_now, denominator = layer_data
        net_flux = (1.0 - albedo_now) * (beam + diffuse)
        new_beam = beam * direct_now
        new_diffuse = (pass_now * diffuse + 0.5 * omega * (1.0 - direct_now) * beam) / denominator
        return (new_beam, new_diffuse), jnp.sum(net_flux, axis=0)

    top_beam = solar_weight[:, None] * cosine[None, :]
    (beam, diffuse), net_sums = lax.scan(downward, (top_beam, jnp.zeros_like(top_beam)), (stack_albedo, passing, unscattered, denominators), unroll=8)
    bottom_down = beam + diffuse
    bottom_net = jnp.sum((1.0 - ground[None, :]) * bottom_down, axis=0)
    interfaces = jnp.concatenate([net_sums, bottom_net[None, :]], axis=0)
    heating = heat_factor * (interfaces[:-1] - interfaces[1:])
    return heating, jnp.sum(bottom_down, axis=0)


def reference(gas_amounts, layer_mass, column_state, absorption, single_scatter, solar_weight, sunlit):
    coefficients = absorption.astype(jnp.float32)

    def one_block(block_data):
        block_gas, block_mass, block_state, block_flag = block_data
        optical = jnp.einsum("gs,lsc->lgc", coefficients, block_gas.astype(jnp.float32))
        heating, surface_down = layer_solve(optical, block_mass.astype(jnp.float32), block_state[0].astype(jnp.float32), block_state[1].astype(jnp.float32), single_scatter, solar_weight)
        heating = jnp.where(block_flag == 1, heating, jnp.zeros_like(heating))
        surface_down = jnp.where(block_flag == 1, surface_down, jnp.zeros_like(surface_down))
        return heating, surface_down

    heating, surface_down = lax.map(one_block, (gas_amounts, layer_mass, column_state, sunlit))
    return (heating, surface_down)
```

```python
import functools
import math

import jax
import jax.numpy as jnp
from jax import lax
from jax.experimental import pallas as pl
from jax.experimental.pallas import tpu as pltpu
from jax.sharding import PartitionSpec as P

MESH = pl.DeviceIdType.MESH
LOG2E = math.log2(math.e)
CHUNK = 8


def gather_kernel(subs, table_ref, omega_ref, weight_ref, table_out, omega_out, weight_out, send_sem, recv_sem):
    band = lax.axis_index("band")
    sub = lax.axis_index("sub")
    barrier = pltpu.get_barrier_semaphore()
    for step in range(1, subs):
        pl.semaphore_signal(barrier, inc=1, device_id=(band, lax.rem(sub + step, subs)), device_id_type=MESH)
    pl.semaphore_wait(barrier, subs - 1)
    pairs = ((table_ref, table_out), (omega_ref, omega_out), (weight_ref, weight_out))
    copies = []
    for step in range(1, subs):
        peer = lax.rem(sub + step, subs)
        for k, (source, target) in enumerate(pairs):
            copy = pltpu.make_async_remote_copy(
                src_ref=source,
                dst_ref=target.at[sub],
                send_sem=send_sem.at[step, k],
                recv_sem=recv_sem.at[step, k],
                device_id=(band, peer),
                device_id_type=MESH,
            )
            copy.start()
            copies.append(copy)
    for source, target in pairs:
        target[sub] = source[...]
    for copy in copies:
        copy.wait()


def gather_tables(absorption, single_scatter, solar_weight, subs):
    share, gases = absorption.shape
    vmem = pl.BlockSpec(memory_space=pltpu.VMEM)
    return pl.pallas_call(
        functools.partial(gather_kernel, subs),
        out_shape=(
            jax.ShapeDtypeStruct((subs, share, gases), jnp.bfloat16),
            jax.ShapeDtypeStruct((subs, 1, share), jnp.float32),
            jax.ShapeDtypeStruct((subs, 1, share), jnp.float32),
        ),
        in_specs=[vmem] * 3,
        out_specs=[vmem] * 3,
        scratch_shapes=[pltpu.SemaphoreType.DMA((subs, 3)), pltpu.SemaphoreType.DMA((subs, 3))],
        compiler_params=pltpu.CompilerParams(collective_id=0, has_side_effects=True),
        name="gather_tables",
    )(absorption, single_scatter.reshape(1, share), solar_weight.reshape(1, share))


def as_column(row, length):
    square = jnp.broadcast_to(row, (length, length))
    rows = lax.broadcasted_iota(jnp.int32, (length, length), 0)
    cols = lax.broadcasted_iota(jnp.int32, (length, length), 1)
    return jnp.sum(jnp.where(rows == cols, square, 0.0), axis=1, keepdims=True)


def solve_kernel(
    own, levels, gases, columns, gpoints, subs,
    sunlit_ref, table_ref, omega_ref, weight_ref, gas_hbm, mass_hbm, state_hbm,
    heat_ref, surf_ref,
    gas_v, mass_v, state_v, coef_v, half_v, weight_v, spread_v,
    depth_v, pass_v, albedo_v, inverse_v, net_v, sem,
):
    band = lax.axis_index("band")
    sub = lax.axis_index("sub")
    share = gpoints // subs
    first = sub * own
    inputs = ((gas_hbm, gas_v), (mass_hbm, mass_v), (state_hbm, state_v))
    copies = [
        pltpu.make_async_copy(source.at[pl.ds(first, own)], target, sem.at[k])
        for k, (source, target) in enumerate(inputs)
    ]
    for copy in copies:
        copy.start()

    for s in range(subs):
        rows = pl.ds(s * share, share)
        coef_v[rows, :] = table_ref[s].astype(jnp.float32) * (-LOG2E)
        half_v[rows, :] = jnp.broadcast_to(0.5 * as_column(omega_ref[s], share), (share, columns))
        weight_v[rows, :] = jnp.broadcast_to(as_column(weight_ref[s], share), (share, columns))
    coef = coef_v[...]
    high = coef.astype(jnp.bfloat16)
    rest = coef - high.astype(jnp.float32)
    middle = rest.astype(jnp.bfloat16)
    low = (rest - middle.astype(jnp.float32)).astype(jnp.bfloat16)
    width = CHUNK * gases
    spread_v[...] = jnp.zeros_like(spread_v)
    for k, part in enumerate((high, middle, low)):
        for l in range(CHUNK):
            at = k * width + l * gases
            spread_v[pl.ds(l * gpoints, gpoints), at : at + gases] = part
    for copy in copies:
        copy.wait()

    chunks = levels // CHUNK

    def block(j, carry):
        state = state_v[j].astype(jnp.float32)
        mu = state[0:1, :]
        ground = state[1:2, :]
        slant = jnp.broadcast_to(1.0 / mu, (8, columns))
        slant = jnp.broadcast_to(slant[0:1, :], (gpoints, columns))

        def optical(c):
            amounts = gas_v[j, pl.ds(pl.multiple_of(c * width, width), width), :]
            amounts = jnp.concatenate([amounts] * 3, axis=0)
            depth = jnp.dot(spread_v[...], amounts, preferred_element_type=jnp.float32)
            depth_v[pl.ds(c * CHUNK, CHUNK)] = depth.reshape(CHUNK, gpoints, columns)

        def upward(i, albedo):
            c = chunks - 1 - i
            optical(c)
            for k in range(CHUNK - 1, -1, -1):
                l = c * CHUNK + k
                half = half_v[...]
                passing = jnp.exp2(depth_v[l])
                square = passing * passing
                reflected = half - half * square
                inverse = 1.0 / (1.0 - reflected * albedo)
                albedo = reflected + square * (albedo * inverse)
                pass_v[l] = passing
                albedo_v[l] = albedo
                inverse_v[l] = inverse
            return albedo

        surface = jnp.broadcast_to(ground, (gpoints, columns))
        lax.fori_loop(0, chunks, upward, surface)

        def downward(c, carry):
            beam, diffuse = carry
            for k in range(CHUNK):
                l = c * CHUNK + k
                half = half_v[...]
                total = (1.0 - albedo_v[l]) * (beam + diffuse)
                net_v[pl.ds(pl.multiple_of(l * 8, 8), 8), :] = jnp.sum(
                    total.reshape(gpoints // 8, 8, columns), axis=0
                )
                beam_next = beam * jnp.exp2(depth_v[l] * slant)
                diffuse = (pass_v[l] * diffuse + half * (beam - beam_next)) * inverse_v[l]
                beam = beam_next
            return beam, diffuse

        top = weight_v[...] * jnp.broadcast_to(mu, (gpoints, columns))
        beam, diffuse = lax.fori_loop(0, chunks, downward, (top, jnp.zeros_like(top)))
        down = jnp.sum((beam + diffuse).reshape(gpoints // 8, 8, columns), axis=0)
        net_v[pl.ds(levels * 8, 8), :] = down * (1.0 - jnp.broadcast_to(ground, (8, columns)))
        here = net_v[pl.ds(0, levels, stride=8), :]
        below = net_v[pl.ds(8, levels, stride=8), :]
        for s in range(1, 8):
            here = here + net_v[pl.ds(s, levels, stride=8), :]
            below = below + net_v[pl.ds(8 + s, levels, stride=8), :]
        lit = sunlit_ref[(band * subs + sub) * own + j] == 1
        heating = mass_v[j].astype(jnp.float32) * (here - below)
        heat_ref[j] = jnp.where(lit, heating, jnp.zeros_like(heating))
        surface_down = jnp.sum(down, axis=0, keepdims=True)
        surf_ref[pl.ds(j, 1), :] = jnp.where(lit, surface_down, jnp.zeros_like(surface_down))
        return carry

    lax.fori_loop(0, own, block, 0)


def solve(gas_amounts, layer_mass, column_state, tables, sunlit, subs):
    blocks, levels, gases, columns = gas_amounts.shape
    own = blocks // subs
    gpoints = tables[0].shape[0] * tables[0].shape[1]
    vmem = pl.BlockSpec(memory_space=pltpu.VMEM)
    anywhere = pl.BlockSpec(memory_space=pl.ANY)
    per_level = pltpu.VMEM((levels, gpoints, columns), jnp.float32)
    return pl.pallas_call(
        functools.partial(solve_kernel, own, levels, gases, columns, gpoints, subs),
        out_shape=(
            jax.ShapeDtypeStruct((own, levels, columns), jnp.float32),
            jax.ShapeDtypeStruct((own, columns), jnp.float32),
        ),
        in_specs=[pl.BlockSpec(memory_space=pltpu.SMEM)] + [vmem] * 3 + [anywhere] * 3,
        out_specs=[vmem] * 2,
        scratch_shapes=[
            pltpu.VMEM((own, levels * gases, columns), jnp.bfloat16),
            pltpu.VMEM((own, levels, columns), jnp.bfloat16),
            pltpu.VMEM((own, 2, columns), jnp.bfloat16),
            pltpu.VMEM((gpoints, gases), jnp.float32),
            pltpu.VMEM((gpoints, columns), jnp.float32),
            pltpu.VMEM((gpoints, columns), jnp.float32),
            pltpu.VMEM((CHUNK * gpoints, 3 * CHUNK * gases), jnp.bfloat16),
            per_level, per_level, per_level, per_level,
            pltpu.VMEM(((levels + 1) * 8, columns), jnp.float32),
            pltpu.SemaphoreType.DMA((3,)),
        ],
        compiler_params=pltpu.CompilerParams(vmem_limit_bytes=48 * 1024 * 1024),
        name="solve_blocks",
    )(sunlit, *tables, gas_amounts.reshape(blocks, levels * gases, columns), layer_mass, column_state)


def body(gas_amounts, layer_mass, column_state, absorption, single_scatter, solar_weight, sunlit):
    subs = lax.axis_size("sub")
    tables = gather_tables(absorption, single_scatter, solar_weight, subs)
    return solve(gas_amounts, layer_mass, column_state, tables, sunlit, subs)


def solution(mesh):
    in_specs = (
        P("band", None, None, None),
        P("band", None, None),
        P("band", None, None),
        P("sub", None),
        P("sub"),
        P("sub"),
        P(),
    )
    out_specs = (P(("band", "sub"), None, None), P(("band", "sub"), None))
    return jax.shard_map(body, mesh=mesh, in_specs=in_specs, out_specs=out_specs, check_vma=False)
```

```python
import functools
import math

import jax
import jax.numpy as jnp
from jax import lax
from jax.experimental import pallas as pl
from jax.experimental.pallas import tpu as pltpu
from jax.sharding import PartitionSpec as P

MESH = pl.DeviceIdType.MESH
LOG2E = math.log2(math.e)
CHUNK = 8
STEP = 16
UP = 4


def kernel(
    own, levels, gases, columns, gpoints, subs,
    gas_hbm, mass_hbm, state_hbm, table_hbm, omega_hbm, weight_hbm, sunlit_hbm,
    heat_hbm, surf_hbm,
    sunlit_s, gas_v, mass_v, state_v, table_v, omega_v, weight_v, lay_v, half_v, top_v, spread_v, coef_v,
    depth_0, depth_1, pass_v, albedo_v, inverse_v, net_v, flux_v, heat_v, surf_v,
    gas_sem, in_sem, out_sem, send_sem, recv_sem,
):
    band = lax.axis_index("band")
    sub = lax.axis_index("sub")
    share = gpoints // subs
    tiles = gpoints // 8
    steps = levels // STEP
    dots = STEP // CHUNK
    width = CHUNK * gases
    first = sub * own

    tables = ((table_hbm, table_v), (omega_hbm, omega_v), (weight_hbm, weight_v))
    own_tables = [
        pltpu.make_async_copy(source, target.at[sub], in_sem.at[k]) for k, (source, target) in enumerate(tables)
    ]
    for copy in own_tables:
        copy.start()
    barrier = pltpu.get_barrier_semaphore()
    for step in range(1, subs):
        pl.semaphore_signal(barrier, inc=1, device_id=(band, lax.rem(sub + step, subs)), device_id_type=MESH)

    def gas_copy(j):
        return pltpu.make_async_copy(gas_hbm.at[first + j], gas_v.at[j], gas_sem.at[j])

    others = [
        pltpu.make_async_copy(state_hbm.at[pl.ds(first, own)], state_v, in_sem.at[3]),
        pltpu.make_async_copy(mass_hbm.at[pl.ds(first, own)], mass_v, in_sem.at[4]),
        pltpu.make_async_copy(sunlit_hbm, sunlit_s, in_sem.at[5]),
    ]
    for j in range(own):
        gas_copy(j).start()
    for copy in others:
        copy.start()
    lay_v[...] = jnp.zeros_like(lay_v)
    spread_v[...] = jnp.zeros_like(spread_v)
    for copy in own_tables:
        copy.wait()
    pl.semaphore_wait(barrier, subs - 1)
    sent = []
    for step in range(1, subs):
        for k, (_, held) in enumerate(tables):
            copy = pltpu.make_async_remote_copy(
                src_ref=held.at[sub],
                dst_ref=held.at[sub],
                send_sem=send_sem.at[step, k],
                recv_sem=recv_sem.at[step, k],
                device_id=(band, lax.rem(sub + step, subs)),
                device_id_type=MESH,
            )
            copy.start()
            sent.append(copy)
    for copy in others:
        copy.wait()
    gas_copy(0).wait()
    for copy in sent:
        copy.wait()

    for s in range(subs):
        at = slice(s * share, (s + 1) * share)
        lay_v[0:gases, at] = table_v[s].astype(jnp.float32)
        lay_v[gases : gases + 1, at] = omega_v[s]
        lay_v[gases + 1 : gases + 2, at] = weight_v[s]
    by_row = jnp.transpose(lay_v[...])[:gpoints]
    coef = by_row[:, :gases] * (-LOG2E)
    half_v[...] = jnp.broadcast_to(0.5 * by_row[:, gases : gases + 1], (gpoints, columns))
    top_v[...] = jnp.broadcast_to(by_row[:, gases + 1 : gases + 2], (gpoints, columns))
    high = coef.astype(jnp.bfloat16).astype(jnp.float32)
    middle = (coef - high).astype(jnp.bfloat16).astype(jnp.float32)
    low = coef - high - middle
    for k, part in enumerate((high, middle, low)):
        for l in range(CHUNK):
            at = k * width + l * gases
            spread_v[pl.ds(l * gpoints, gpoints), at : at + gases] = part
    coef_v[...] = spread_v[...].astype(jnp.bfloat16)

    depths = (depth_0, depth_1)

    def state_row(j, k):
        row = state_v[j].astype(jnp.float32)[k : k + 1, :]
        return jnp.broadcast_to(row, (8, columns))

    def all_rows(row):
        return jnp.broadcast_to(row[None], (tiles, 8, columns)).reshape(gpoints, columns)

    def optical(j, slot, i):
        amounts = jnp.concatenate(
            [gas_v[j, pl.ds(pl.multiple_of((i * dots + d) * width, width), width), :] for d in range(dots)], axis=1
        )
        amounts = jnp.concatenate([amounts] * 3, axis=0)
        depth = jnp.dot(coef_v[...], amounts, preferred_element_type=jnp.float32)
        for d in range(dots):
            for m in range(CHUNK):
                part = depth[m * gpoints : (m + 1) * gpoints, d * columns : (d + 1) * columns]
                depths[slot][i * STEP + d * CHUNK + m] = part

    def upward(j, slot):
        def body(i, albedo):
            half = half_v[...]
            for k in range(UP):
                l = levels - 1 - (i * UP + k)
                passing = jnp.exp2(depths[slot][l])
                pass_v[l] = passing
                square = passing * passing
                reflected = half - half * square
                inverse = 1.0 / (1.0 - reflected * albedo)
                albedo = reflected + (square * albedo) * inverse
                albedo_v[l] = albedo
                inverse_v[l] = inverse
            return albedo

        lax.fori_loop(0, levels // UP, body, all_rows(state_row(j, 1)))

    def downward(j, slot, j_next):
        top = top_v[...] * all_rows(state_row(j, 0))
        slant = all_rows(1.0 / state_row(j, 0))

        def body(i, carry):
            beam, diffuse = carry
            half = half_v[...]
            if j_next is not None:
                optical(j_next, 1 - slot, i)
            for k in range(STEP):
                l = i * STEP + k
                net = (1.0 - albedo_v[l]) * (beam + diffuse)
                net_v[pl.ds(pl.multiple_of(l * 8, 8), 8), :] = jnp.sum(net.reshape(tiles, 8, columns), axis=0)
                beam_next = beam * jnp.exp2(depths[slot][l] * slant)
                diffuse = (pass_v[l] * diffuse + half * (beam - beam_next)) * inverse_v[l]
                beam = beam_next
            return beam, diffuse

        beam, diffuse = lax.fori_loop(0, steps, body, (top, jnp.zeros_like(top)))
        net_v[pl.ds(levels * 8, 8), :] = jnp.sum((beam + diffuse).reshape(tiles, 8, columns), axis=0)

    def heat_copy(j):
        return pltpu.make_async_copy(heat_v.at[j], heat_hbm.at[j], out_sem.at[j])

    def finish(j):
        at = pl.ds(levels * 8, 8)
        bottom = net_v[at, :]
        net_v[at, :] = bottom * (1.0 - state_row(j, 1))
        here = net_v[pl.ds(0, levels, stride=8), :]
        for s in range(1, 8):
            here = here + net_v[pl.ds(s, levels, stride=8), :]
        flux_v[pl.ds(0, levels), :] = here
        flux_v[pl.ds(levels, 1), :] = jnp.sum(net_v[at, :], axis=0, keepdims=True)
        below = flux_v[pl.ds(1, levels), :]
        lit = sunlit_s[(band * subs + sub) * own + j] == 1
        heating = mass_v[j].astype(jnp.float32) * (here - below)
        heat_v[j] = jnp.where(lit, heating, jnp.zeros_like(heating))
        heat_copy(j).start()
        surface_down = jnp.sum(bottom, axis=0, keepdims=True)
        surf_v[pl.ds(j, 1), :] = jnp.where(lit, surface_down, jnp.zeros_like(surface_down))

    lax.fori_loop(0, steps, lambda i, c: (optical(0, 0, i), c)[1], 0)

    def pair(p, carry):
        for slot in range(2):
            j = p * 2 + slot
            upward(j, slot)
            gas_copy(j + 1).wait()
            downward(j, slot, j + 1)
            finish(j)
        return carry

    lax.fori_loop(0, own // 2 - 1, pair, 0)
    for slot in range(2):
        j = own - 2 + slot
        upward(j, slot)
        if slot == 0:
            gas_copy(j + 1).wait()
        downward(j, slot, None if slot else j + 1)
        finish(j)
    surf_copy = pltpu.make_async_copy(surf_v, surf_hbm, in_sem.at[0])
    surf_copy.start()
    for j in range(own):
        heat_copy(j).wait()
    surf_copy.wait()


def body(gas_amounts, layer_mass, column_state, absorption, single_scatter, solar_weight, sunlit):
    subs = lax.axis_size("sub")
    blocks, levels, gases, columns = gas_amounts.shape
    share = absorption.shape[0]
    own, gpoints = blocks // subs, share * subs
    anywhere = pl.BlockSpec(memory_space=pl.ANY)
    per_level = pltpu.VMEM((levels, gpoints, columns), jnp.float32)
    net = pltpu.VMEM(((levels + 1) * 8, columns), jnp.float32)
    return pl.pallas_call(
        functools.partial(kernel, own, levels, gases, columns, gpoints, subs),
        out_shape=(
            jax.ShapeDtypeStruct((own, levels, columns), jnp.float32),
            jax.ShapeDtypeStruct((own, columns), jnp.float32),
        ),
        in_specs=[anywhere] * 7,
        out_specs=[anywhere] * 2,
        scratch_shapes=[
            pltpu.SMEM((sunlit.shape[0],), jnp.int32),
            pltpu.VMEM((own, levels * gases, columns), jnp.bfloat16),
            pltpu.VMEM((own, levels, columns), jnp.bfloat16),
            pltpu.VMEM((own, 2, columns), jnp.bfloat16),
            pltpu.VMEM((subs, gases, share), jnp.bfloat16),
            pltpu.VMEM((subs, 1, share), jnp.float32),
            pltpu.VMEM((subs, 1, share), jnp.float32),
            pltpu.VMEM((16, 128), jnp.float32),
            pltpu.VMEM((gpoints, columns), jnp.float32),
            pltpu.VMEM((gpoints, columns), jnp.float32),
            pltpu.VMEM((CHUNK * gpoints, 3 * CHUNK * gases), jnp.float32),
            pltpu.VMEM((CHUNK * gpoints, 3 * CHUNK * gases), jnp.bfloat16),
        ]
        + [per_level] * 5
        + [
            net,
            pltpu.VMEM((levels + 8, columns), jnp.float32),
            pltpu.VMEM((own, levels, columns), jnp.float32),
            pltpu.VMEM((own, columns), jnp.float32),
            pltpu.SemaphoreType.DMA((own,)),
            pltpu.SemaphoreType.DMA((6,)),
            pltpu.SemaphoreType.DMA((own,)),
            pltpu.SemaphoreType.DMA((subs, 3)),
            pltpu.SemaphoreType.DMA((subs, 3)),
        ],
        compiler_params=pltpu.CompilerParams(
            collective_id=0, has_side_effects=True, vmem_limit_bytes=60 * 1024 * 1024
        ),
        name="solve_blocks",
    )(
        gas_amounts.reshape(blocks, levels * gases, columns),
        layer_mass,
        column_state,
        absorption.T,
        single_scatter.reshape(1, share),
        solar_weight.reshape(1, share),
        sunlit,
    )


def solution(mesh):
    in_specs = (
        P("band", None, None, None),
        P("band", None, None),
        P("band", None, None),
        P("sub", None),
        P("sub"),
        P("sub"),
        P(),
    )
    out_specs = (P(("band", "sub"), None, None), P(("band", "sub"), None))
    return jax.shard_map(body, mesh=mesh, in_specs=in_specs, out_specs=out_specs, check_vma=False)
```

```python
import functools
import math

import jax
import jax.numpy as jnp
from jax import lax
from jax.experimental import pallas as pl
from jax.experimental.pallas import tpu as pltpu
from jax.sharding import PartitionSpec as P

MESH = pl.DeviceIdType.MESH
LOG2E = math.log2(math.e)
CHUNK = 8
STEP = 32
GROUPS = 2


def exchange_kernel(gases, share, subs, table_hbm, omega_hbm, weight_hbm, packed_hbm, table_v, omega_v, weight_v, pack_v, in_sem, send_sem, recv_sem):
    band = lax.axis_index("band")
    sub = lax.axis_index("sub")
    barrier = pltpu.get_barrier_semaphore()
    for step in range(1, subs):
        pl.semaphore_signal(barrier, inc=1, device_id=(band, lax.rem(sub + step, subs)), device_id_type=MESH)
    tables = ((table_hbm, table_v), (omega_hbm, omega_v), (weight_hbm, weight_v))
    copies = [pltpu.make_async_copy(source, target, in_sem.at[k]) for k, (source, target) in enumerate(tables)]
    for copy in copies:
        copy.start()
    for copy in copies:
        copy.wait()
    pack_v[0:gases, 0:share] = table_v[...].astype(jnp.float32)
    pack_v[0:1, 32 : 32 + share] = omega_v[...]
    pack_v[0:1, 64 : 64 + share] = weight_v[...]
    pl.semaphore_wait(barrier, subs - 1)
    sent = []
    for step in range(1, subs):
        copy = pltpu.make_async_remote_copy(
            src_ref=pack_v,
            dst_ref=packed_hbm.at[sub],
            send_sem=send_sem.at[step],
            recv_sem=recv_sem.at[step],
            device_id=(band, lax.rem(sub + step, subs)),
            device_id_type=MESH,
        )
        copy.start()
        sent.append(copy)
    own_part = pltpu.make_async_copy(pack_v, packed_hbm.at[sub], in_sem.at[0])
    own_part.start()
    own_part.wait()
    for copy in sent:
        copy.wait()


def exchange(absorption, single_scatter, solar_weight, subs):
    share, gases = absorption.shape
    anywhere = pl.BlockSpec(memory_space=pl.ANY)
    return pl.pallas_call(
        functools.partial(exchange_kernel, gases, share, subs),
        out_shape=jax.ShapeDtypeStruct((subs, 8, 128), jnp.float32),
        in_specs=[anywhere] * 3,
        out_specs=anywhere,
        scratch_shapes=[
            pltpu.VMEM((gases, share), jnp.bfloat16),
            pltpu.VMEM((1, share), jnp.float32),
            pltpu.VMEM((1, share), jnp.float32),
            pltpu.VMEM((8, 128), jnp.float32),
            pltpu.SemaphoreType.DMA((3,)),
            pltpu.SemaphoreType.DMA((subs,)),
            pltpu.SemaphoreType.DMA((subs,)),
        ],
        compiler_params=pltpu.CompilerParams(collective_id=0, has_side_effects=True),
        name="exchange_tables",
    )(absorption.T, single_scatter.reshape(1, share), solar_weight.reshape(1, share))


def kernel(
    own, levels, gases, columns, gpoints, subs,
    gas_hbm, mass_hbm, state_hbm, packed_hbm, sunlit_hbm,
    heat_hbm, surf_hbm,
    sunlit_s, gas_v, mass_v, state_v, pack_v, lay_v, half_v, top_v, spread_v, coef_v,
    depth_00, depth_01, depth_10, depth_11, pass_0, pass_1, upper_0, upper_1, lower_0, lower_1, net_0, net_v, flux_v, heat_v, surf_v,
    gas_sem, in_sem, out_sem,
):
    band = lax.axis_index("band")
    sub = lax.axis_index("sub")
    share = gpoints // subs
    rows = gpoints // GROUPS
    tiles = rows // 8
    steps = levels // STEP
    dots = STEP // CHUNK
    width = CHUNK * gases
    first = sub * own

    packed_copy = pltpu.make_async_copy(packed_hbm, pack_v, in_sem.at[1])
    packed_copy.start()

    def gas_copy(j):
        return pltpu.make_async_copy(gas_hbm.at[first + j], gas_v.at[j], gas_sem.at[j])

    others = [
        pltpu.make_async_copy(state_hbm.at[pl.ds(first, own)], state_v, in_sem.at[3]),
        pltpu.make_async_copy(mass_hbm.at[pl.ds(first, own)], mass_v, in_sem.at[4]),
        pltpu.make_async_copy(sunlit_hbm, sunlit_s, in_sem.at[5]),
    ]
    for j in range(own):
        gas_copy(j).start()
    for copy in others:
        copy.start()
    lay_v[...] = jnp.zeros_like(lay_v)
    spread_v[...] = jnp.zeros_like(spread_v)
    packed_copy.wait()
    for copy in others:
        copy.wait()
    gas_copy(0).wait()

    for s in range(subs):
        at = slice(s * share, (s + 1) * share)
        lay_v[0:gases, at] = pack_v[s, 0:gases, 0:share]
        lay_v[gases : gases + 1, at] = pack_v[s, 0:1, 32 : 32 + share]
        lay_v[gases + 1 : gases + 2, at] = pack_v[s, 0:1, 64 : 64 + share]
    by_row = jnp.transpose(lay_v[...])[:gpoints]
    coef = by_row[:, :gases] * (-LOG2E)
    half_v[...] = jnp.broadcast_to(0.5 * by_row[:, gases : gases + 1], (gpoints, columns))
    top_v[...] = jnp.broadcast_to(by_row[:, gases + 1 : gases + 2], (gpoints, columns))
    high = coef.astype(jnp.bfloat16).astype(jnp.float32)
    middle = (coef - high).astype(jnp.bfloat16).astype(jnp.float32)
    low = coef - high - middle
    for k, part in enumerate((high, middle, low)):
        for g in range(GROUPS):
            for l in range(CHUNK):
                at = k * width + l * gases
                spread_v[pl.ds((g * CHUNK + l) * rows, rows), at : at + gases] = part[g * rows : (g + 1) * rows]
    coef_v[...] = spread_v[...].astype(jnp.bfloat16)

    depths = ((depth_00, depth_01), (depth_10, depth_11))
    passes, uppers, lowers, nets = (pass_0, pass_1), (upper_0, upper_1), (lower_0, lower_1), (net_0, net_v)

    def state_row(j, k):
        row = state_v[j].astype(jnp.float32)[k : k + 1, :]
        return jnp.broadcast_to(row, (8, columns))

    def all_rows(row):
        return jnp.broadcast_to(row[None], (tiles, 8, columns)).reshape(rows, columns)

    def optical(j, slot, g, i):
        amounts = jnp.concatenate(
            [gas_v[j, pl.ds(pl.multiple_of((i * dots + d) * width, width), width), :] for d in range(dots)], axis=1
        )
        amounts = jnp.concatenate([amounts] * 3, axis=0)
        return jnp.dot(coef_v[pl.ds(g * CHUNK * rows, CHUNK * rows), :], amounts, preferred_element_type=jnp.float32)

    def keep(depth, slot, g, i):
        for d in range(dots):
            for m in range(CHUNK):
                part = depth[m * rows : (m + 1) * rows, d * columns : (d + 1) * columns]
                depths[slot][g][i * STEP + d * CHUNK + m] = part

    def run(down, up, coming):
        start = ()
        if up is not None:
            ground = all_rows(state_row(up[0], 1))
            start += (ground, jnp.ones_like(ground))
        if down is not None:
            mu = all_rows(state_row(down[0], 0))
            slant = 1.0 / mu
            top = top_v[pl.ds(down[2] * rows, rows), :] * mu
            start += (top, jnp.zeros_like(top))

        def body(i, carry):
            carry = list(carry)
            if coming is not None:
                ready = optical(*coming, i)
            if up is not None:
                _, slot, g = up
                upper, lower = carry[:2]
                half_up = half_v[pl.ds(g * rows, rows), :]
            if down is not None:
                _, slot_d, g_d = down
                beam, scaled = carry[-2:]
                half_down = half_v[pl.ds(g_d * rows, rows), :]
            for k in range(STEP):
                if up is not None:
                    l = levels - 1 - (i * STEP + k)
                    passing = jnp.exp2(depths[slot][g][l])
                    passes[g][l] = passing
                    square = passing * passing
                    reflected = half_up - half_up * square
                    lower = lower - reflected * upper
                    upper = reflected * lower + square * upper
                    uppers[g][l] = upper
                    lowers[g][l] = lower
                if down is not None:
                    l = i * STEP + k
                    below = lowers[g_d][l]
                    inverse = 1.0 / below
                    net = (below - uppers[g_d][l]) * (beam * inverse + scaled)
                    at = pl.ds(pl.multiple_of(l * 8, 8), 8)
                    net = jnp.sum(net.reshape(tiles, 8, columns), axis=0)
                    nets[g_d][at, :] = net if g_d == 0 else net + nets[0][at, :]
                    beam_next = beam * jnp.exp2(depths[slot_d][g_d][l] * slant)
                    scaled = passes[g_d][l] * scaled + (half_down * (beam - beam_next)) * inverse
                    beam = beam_next
            if coming is not None:
                keep(ready, *coming[1:], i)
            return (() if up is None else (upper, lower)) + (() if down is None else (beam, scaled))

        end = lax.fori_loop(0, steps, body, start)
        if down is not None:
            beam, diffuse = end[-2:]
            at = pl.ds(levels * 8, 8)
            net = jnp.sum((beam + diffuse).reshape(tiles, 8, columns), axis=0)
            nets[down[2]][at, :] = net if down[2] == 0 else net + nets[0][at, :]

    def heat_copy(j):
        return pltpu.make_async_copy(heat_v.at[j], heat_hbm.at[j], out_sem.at[j])

    def finish(j):
        at = pl.ds(levels * 8, 8)
        bottom = net_v[at, :]
        net_v[at, :] = bottom * (1.0 - state_row(j, 1))
        here = net_v[pl.ds(0, levels, stride=8), :]
        for s in range(1, 8):
            here = here + net_v[pl.ds(s, levels, stride=8), :]
        flux_v[pl.ds(0, levels), :] = here
        flux_v[pl.ds(levels, 1), :] = jnp.sum(net_v[at, :], axis=0, keepdims=True)
        below = flux_v[pl.ds(1, levels), :]
        lit = sunlit_s[(band * subs + sub) * own + j] == 1
        heating = mass_v[j].astype(jnp.float32) * (here - below)
        heat_v[j] = jnp.where(lit, heating, jnp.zeros_like(heating))
        heat_copy(j).start()
        surface_down = jnp.sum(bottom, axis=0, keepdims=True)
        surf_v[pl.ds(j, 1), :] = jnp.where(lit, surface_down, jnp.zeros_like(surface_down))

    def prepare(i, carry):
        for g in range(GROUPS):
            keep(optical(0, 0, g, i), 0, g, i)
        return carry

    lax.fori_loop(0, steps, prepare, 0)
    run(None, (0, 0, 0), None)

    def pair(p, carry):
        for slot in range(2):
            j = p * 2 + slot
            other = 1 - slot
            gas_copy(j + 1).wait()
            run((j, slot, 0), (j, slot, 1), (j + 1, other, 0))
            run((j, slot, 1), (j + 1, other, 0), (j + 1, other, 1))
            finish(j)
        return carry

    lax.fori_loop(0, own // 2 - 1, pair, 0)
    j = own - 2
    gas_copy(j + 1).wait()
    run((j, 0, 0), (j, 0, 1), (j + 1, 1, 0))
    run((j, 0, 1), (j + 1, 1, 0), (j + 1, 1, 1))
    finish(j)
    run((j + 1, 1, 0), (j + 1, 1, 1), None)
    run((j + 1, 1, 1), None, None)
    finish(j + 1)
    surf_copy = pltpu.make_async_copy(surf_v, surf_hbm, in_sem.at[0])
    surf_copy.start()
    for j in range(own):
        heat_copy(j).wait()
    surf_copy.wait()


def body(gas_amounts, layer_mass, column_state, absorption, single_scatter, solar_weight, sunlit):
    subs = lax.axis_size("sub")
    blocks, levels, gases, columns = gas_amounts.shape
    share = absorption.shape[0]
    own, gpoints = blocks // subs, share * subs
    anywhere = pl.BlockSpec(memory_space=pl.ANY)
    per_level = pltpu.VMEM((levels, gpoints // GROUPS, columns), jnp.float32)
    net = pltpu.VMEM(((levels + 1) * 8, columns), jnp.float32)
    return pl.pallas_call(
        functools.partial(kernel, own, levels, gases, columns, gpoints, subs),
        out_shape=(
            jax.ShapeDtypeStruct((own, levels, columns), jnp.float32),
            jax.ShapeDtypeStruct((own, columns), jnp.float32),
        ),
        in_specs=[anywhere] * 5,
        out_specs=[anywhere] * 2,
        scratch_shapes=[
            pltpu.SMEM((sunlit.shape[0],), jnp.int32),
            pltpu.VMEM((own, levels * gases, columns), jnp.bfloat16),
            pltpu.VMEM((own, levels, columns), jnp.bfloat16),
            pltpu.VMEM((own, 2, columns), jnp.bfloat16),
            pltpu.VMEM((subs, 8, 128), jnp.float32),
            pltpu.VMEM((16, 128), jnp.float32),
            pltpu.VMEM((gpoints, columns), jnp.float32),
            pltpu.VMEM((gpoints, columns), jnp.float32),
            pltpu.VMEM((CHUNK * gpoints, 3 * CHUNK * gases), jnp.float32),
            pltpu.VMEM((CHUNK * gpoints, 3 * CHUNK * gases), jnp.bfloat16),
        ]
        + [per_level] * 10
        + [
            net, net,
            pltpu.VMEM((levels + 8, columns), jnp.float32),
            pltpu.VMEM((own, levels, columns), jnp.float32),
            pltpu.VMEM((own, columns), jnp.float32),
            pltpu.SemaphoreType.DMA((own,)),
            pltpu.SemaphoreType.DMA((6,)),
            pltpu.SemaphoreType.DMA((own,)),
        ],
        compiler_params=pltpu.CompilerParams(
            vmem_limit_bytes=60 * 1024 * 1024
        ),
        name="solve_blocks",
    )(
        gas_amounts.reshape(blocks, levels * gases, columns),
        layer_mass,
        column_state,
        exchange(absorption, single_scatter, solar_weight, subs),
        sunlit,
    )


def solution(mesh):
    in_specs = (
        P("band", None, None, None),
        P("band", None, None),
        P("band", None, None),
        P("sub", None),
        P("sub"),
        P("sub"),
        P(),
    )
    out_specs = (P(("band", "sub"), None, None), P(("band", "sub"), None))
    return jax.shard_map(body, mesh=mesh, in_specs=in_specs, out_specs=out_specs, check_vma=False)
```

```python
import functools
import math

import jax
import jax.numpy as jnp
from jax import lax
from jax.experimental import pallas as pl
from jax.experimental.pallas import tpu as pltpu
from jax.sharding import PartitionSpec as P

MESH = pl.DeviceIdType.MESH
LOG2E = math.log2(math.e)
CHUNK = 8
STEP = 32
GROUPS = 2


def exchange_kernel(
    own, levels, gases, columns, share, subs,
    gas_hbm, mass_hbm, state_hbm, table_hbm, omega_hbm, weight_hbm,
    gas_out, mass_out, state_out, coef_out, half_out, top_out,
    table_v, omega_v, weight_v, pack_v, lay_v, spread_v, in_sem, send_sem, recv_sem,
):
    band = lax.axis_index("band")
    sub = lax.axis_index("sub")
    gpoints = share * subs
    rows = gpoints // GROUPS
    width = CHUNK * gases
    barrier = pltpu.get_barrier_semaphore()
    for step in range(1, subs):
        pl.semaphore_signal(barrier, inc=1, device_id=(band, lax.rem(sub + step, subs)), device_id_type=MESH)
    tables = ((table_hbm, table_v), (omega_hbm, omega_v), (weight_hbm, weight_v))
    copies = [pltpu.make_async_copy(source, target, in_sem.at[k]) for k, (source, target) in enumerate(tables)]
    blocks = ((gas_hbm, gas_out), (mass_hbm, mass_out), (state_hbm, state_out))
    others = [
        pltpu.make_async_copy(source.at[pl.ds(sub * own, own)], target, in_sem.at[3 + k])
        for k, (source, target) in enumerate(blocks)
    ]
    for copy in copies + others:
        copy.start()
    lay_v[...] = jnp.zeros_like(lay_v)
    spread_v[...] = jnp.zeros_like(spread_v)
    for copy in copies:
        copy.wait()
    pack_v[sub, 0:gases, 0:share] = table_v[...].astype(jnp.float32)
    pack_v[sub, 0:1, 32 : 32 + share] = omega_v[...]
    pack_v[sub, 0:1, 64 : 64 + share] = weight_v[...]
    pl.semaphore_wait(barrier, subs - 1)
    sent = []
    for step in range(1, subs):
        copy = pltpu.make_async_remote_copy(
            src_ref=pack_v.at[sub],
            dst_ref=pack_v.at[sub],
            send_sem=send_sem.at[step],
            recv_sem=recv_sem.at[step],
            device_id=(band, lax.rem(sub + step, subs)),
            device_id_type=MESH,
        )
        copy.start()
        sent.append(copy)
    for copy in others:
        copy.wait()
    for copy in sent:
        copy.wait()

    for s in range(subs):
        at = slice(s * share, (s + 1) * share)
        lay_v[0:gases, at] = pack_v[s, 0:gases, 0:share]
        lay_v[gases : gases + 1, at] = pack_v[s, 0:1, 32 : 32 + share]
        lay_v[gases + 1 : gases + 2, at] = pack_v[s, 0:1, 64 : 64 + share]
    by_row = jnp.transpose(lay_v[...])[:gpoints]
    coef = by_row[:, :gases] * (-LOG2E)
    half_out[...] = jnp.broadcast_to(0.5 * by_row[:, gases : gases + 1], (gpoints, columns))
    top_out[...] = jnp.broadcast_to(by_row[:, gases + 1 : gases + 2], (gpoints, columns))
    high = coef.astype(jnp.bfloat16).astype(jnp.float32)
    middle = (coef - high).astype(jnp.bfloat16).astype(jnp.float32)
    low = coef - high - middle
    for k, part in enumerate((high, middle, low)):
        for g in range(GROUPS):
            for l in range(CHUNK):
                at = k * width + l * gases
                spread_v[pl.ds((g * CHUNK + l) * rows, rows), at : at + gases] = part[g * rows : (g + 1) * rows]
    coef_out[...] = spread_v[...].astype(jnp.bfloat16)


def exchange(gas, layer_mass, column_state, absorption, single_scatter, solar_weight, subs):
    share, gases = absorption.shape
    blocks, depth, columns = gas.shape
    own, levels, gpoints = blocks // subs, depth // gases, share * subs
    anywhere = pl.BlockSpec(memory_space=pltpu.HBM)
    vmem = pl.BlockSpec(memory_space=pltpu.VMEM)
    return pl.pallas_call(
        functools.partial(exchange_kernel, own, levels, gases, columns, share, subs),
        out_shape=(
            pltpu.VMEM((own, depth, columns), jnp.bfloat16),
            pltpu.VMEM((own, levels, columns), jnp.bfloat16),
            pltpu.VMEM((own, 2, columns), jnp.bfloat16),
            pltpu.VMEM((CHUNK * gpoints, 3 * CHUNK * gases), jnp.bfloat16),
            pltpu.VMEM((gpoints, columns), jnp.float32),
            pltpu.VMEM((gpoints, columns), jnp.float32),
        ),
        in_specs=[anywhere] * 6,
        out_specs=[vmem] * 6,
        scratch_shapes=[
            pltpu.VMEM((gases, share), jnp.bfloat16),
            pltpu.VMEM((1, share), jnp.float32),
            pltpu.VMEM((1, share), jnp.float32),
            pltpu.VMEM((subs, 8, 128), jnp.float32),
            pltpu.VMEM((16, 128), jnp.float32),
            pltpu.VMEM((CHUNK * gpoints, 3 * CHUNK * gases), jnp.float32),
            pltpu.SemaphoreType.DMA((6,)),
            pltpu.SemaphoreType.DMA((subs,)),
            pltpu.SemaphoreType.DMA((subs,)),
        ],
        compiler_params=pltpu.CompilerParams(
            collective_id=0, has_side_effects=True, vmem_limit_bytes=65100000
        ),
        name="exchange_tables",
    )(gas, layer_mass, column_state, absorption.T, single_scatter.reshape(1, share), solar_weight.reshape(1, share))


def kernel(
    own, levels, gases, columns, gpoints, subs,
    gas_v, mass_v, state_v, coef_v, half_v, top_v, sunlit_hbm,
    heat_hbm, surf_hbm,
    sunlit_s, depth_00, depth_01, depth_10, depth_11, pass_0, pass_1, upper_0, upper_1, lower_0, lower_1, net_0, net_v, flux_v, heat_v, surf_v,
    in_sem, out_sem,
):
    band = lax.axis_index("band")
    sub = lax.axis_index("sub")
    rows = gpoints // GROUPS
    tiles = rows // 8
    steps = levels // STEP
    dots = STEP // CHUNK
    width = CHUNK * gases

    lit_copy = pltpu.make_async_copy(sunlit_hbm, sunlit_s, in_sem.at[0])
    lit_copy.start()

    depths = ((depth_00, depth_01), (depth_10, depth_11))
    passes, uppers, lowers, nets = (pass_0, pass_1), (upper_0, upper_1), (lower_0, lower_1), (net_0, net_v)

    def state_row(j, k):
        row = state_v[j].astype(jnp.float32)[k : k + 1, :]
        return jnp.broadcast_to(row, (8, columns))

    def all_rows(row):
        return jnp.broadcast_to(row[None], (tiles, 8, columns)).reshape(rows, columns)

    def optical(j, slot, g, i):
        amounts = jnp.concatenate(
            [gas_v[j, pl.ds(pl.multiple_of((i * dots + d) * width, width), width), :] for d in range(dots)], axis=1
        )
        amounts = jnp.concatenate([amounts] * 3, axis=0)
        return jnp.dot(coef_v[pl.ds(g * CHUNK * rows, CHUNK * rows), :], amounts, preferred_element_type=jnp.float32)

    def keep(depth, slot, g, i):
        for d in range(dots):
            for m in range(CHUNK):
                part = depth[m * rows : (m + 1) * rows, d * columns : (d + 1) * columns]
                depths[slot][g][i * STEP + d * CHUNK + m] = part

    def run(down, up, coming):
        start = ()
        if up is not None:
            ground = all_rows(state_row(up[0], 1))
            start += (ground, jnp.ones_like(ground))
        if down is not None:
            mu = all_rows(state_row(down[0], 0))
            slant = 1.0 / mu
            top = top_v[pl.ds(down[2] * rows, rows), :] * mu
            start += (top, jnp.zeros_like(top))

        def body(i, carry):
            carry = list(carry)
            if coming is not None:
                ready = optical(*coming, i)
            if up is not None:
                _, slot, g = up
                upper, lower = carry[:2]
                half_up = half_v[pl.ds(g * rows, rows), :]
            if down is not None:
                _, slot_d, g_d = down
                beam, scaled = carry[-2:]
                half_down = half_v[pl.ds(g_d * rows, rows), :]
            for k in range(STEP):
                if up is not None:
                    l = levels - 1 - (i * STEP + k)
                    passing = jnp.exp2(depths[slot][g][l])
                    passes[g][l] = passing
                    square = passing * passing
                    reflected = half_up - half_up * square
                    lower = lower - reflected * upper
                    upper = reflected * lower + square * upper
                    uppers[g][l] = upper
                    lowers[g][l] = lower
                if down is not None:
                    l = i * STEP + k
                    below = lowers[g_d][l]
                    inverse = 1.0 / below
                    net = (below - uppers[g_d][l]) * (beam * inverse + scaled)
                    at = pl.ds(pl.multiple_of(l * 8, 8), 8)
                    net = jnp.sum(net.reshape(tiles, 8, columns), axis=0)
                    nets[g_d][at, :] = net if g_d == 0 else net + nets[0][at, :]
                    beam_next = beam * jnp.exp2(depths[slot_d][g_d][l] * slant)
                    scaled = passes[g_d][l] * scaled + (half_down * (beam - beam_next)) * inverse
                    beam = beam_next
            if coming is not None:
                keep(ready, *coming[1:], i)
            return (() if up is None else (upper, lower)) + (() if down is None else (beam, scaled))

        end = lax.fori_loop(0, steps, body, start)
        if down is not None:
            beam, diffuse = end[-2:]
            at = pl.ds(levels * 8, 8)
            net = jnp.sum((beam + diffuse).reshape(tiles, 8, columns), axis=0)
            nets[down[2]][at, :] = net if down[2] == 0 else net + nets[0][at, :]

    def heat_copy(j):
        return pltpu.make_async_copy(heat_v.at[j], heat_hbm.at[j], out_sem.at[j])

    def finish(j):
        at = pl.ds(levels * 8, 8)
        bottom = net_v[at, :]
        net_v[at, :] = bottom * (1.0 - state_row(j, 1))
        here = net_v[pl.ds(0, levels, stride=8), :]
        for s in range(1, 8):
            here = here + net_v[pl.ds(s, levels, stride=8), :]
        flux_v[pl.ds(0, levels), :] = here
        flux_v[pl.ds(levels, 1), :] = jnp.sum(net_v[at, :], axis=0, keepdims=True)
        below = flux_v[pl.ds(1, levels), :]
        lit = sunlit_s[(band * subs + sub) * own + j] == 1
        heating = mass_v[j].astype(jnp.float32) * (here - below)
        heat_v[j] = jnp.where(lit, heating, jnp.zeros_like(heating))
        heat_copy(j).start()
        surface_down = jnp.sum(bottom, axis=0, keepdims=True)
        surf_v[pl.ds(j, 1), :] = jnp.where(lit, surface_down, jnp.zeros_like(surface_down))

    def prepare(i, carry):
        keep(optical(0, 0, 0, i), 0, 0, i)
        return carry

    lax.fori_loop(0, steps, prepare, 0)
    run(None, (0, 0, 0), (0, 0, 1))
    lit_copy.wait()

    def pair(p, carry):
        for slot in range(2):
            j = p * 2 + slot
            other = 1 - slot
            run((j, slot, 0), (j, slot, 1), (j + 1, other, 0))
            run((j, slot, 1), (j + 1, other, 0), (j + 1, other, 1))
            finish(j)
        return carry

    lax.fori_loop(0, own // 2 - 1, pair, 0)
    j = own - 2
    run((j, 0, 0), (j, 0, 1), (j + 1, 1, 0))
    run((j, 0, 1), (j + 1, 1, 0), (j + 1, 1, 1))
    finish(j)
    run((j + 1, 1, 0), (j + 1, 1, 1), None)
    run((j + 1, 1, 1), None, None)
    finish(j + 1)
    surf_copy = pltpu.make_async_copy(surf_v, surf_hbm, in_sem.at[1])
    surf_copy.start()
    for j in range(own):
        heat_copy(j).wait()
    surf_copy.wait()


def body(gas_amounts, layer_mass, column_state, absorption, single_scatter, solar_weight, sunlit):
    subs = lax.axis_size("sub")
    blocks, levels, gases, columns = gas_amounts.shape
    share = absorption.shape[0]
    own, gpoints = blocks // subs, share * subs
    anywhere = pl.BlockSpec(memory_space=pltpu.HBM)
    per_level = pltpu.VMEM((levels, gpoints // GROUPS, columns), jnp.float32)
    net = pltpu.VMEM(((levels + 1) * 8, columns), jnp.float32)
    return pl.pallas_call(
        functools.partial(kernel, own, levels, gases, columns, gpoints, subs),
        out_shape=(
            jax.ShapeDtypeStruct((own, levels, columns), jnp.float32),
            jax.ShapeDtypeStruct((own, columns), jnp.float32),
        ),
        in_specs=[pl.BlockSpec(memory_space=pltpu.VMEM)] * 6 + [anywhere],
        out_specs=[anywhere] * 2,
        scratch_shapes=[
            pltpu.SMEM((sunlit.shape[0],), jnp.int32),
        ]
        + [per_level] * 10
        + [
            net, net,
            pltpu.VMEM((levels + 8, columns), jnp.float32),
            pltpu.VMEM((own, levels, columns), jnp.float32),
            pltpu.VMEM((own, columns), jnp.float32),
            pltpu.SemaphoreType.DMA((2,)),
            pltpu.SemaphoreType.DMA((own,)),
        ],
        compiler_params=pltpu.CompilerParams(
            vmem_limit_bytes=40 * 1024 * 1024
        ),
        name="solve_blocks",
    )(
        *exchange(
            gas_amounts.reshape(blocks, levels * gases, columns),
            layer_mass,
            column_state,
            absorption,
            single_scatter,
            solar_weight,
            subs,
        ),
        sunlit,
    )


def solution(mesh):
    in_specs = (
        P("band", None, None, None),
        P("band", None, None),
        P("band", None, None),
        P("sub", None),
        P("sub"),
        P("sub"),
        P(),
    )
    out_specs = (P(("band", "sub"), None, None), P(("band", "sub"), None))
    return jax.shard_map(body, mesh=mesh, in_specs=in_specs, out_specs=out_specs, check_vma=False)
```

```python
import functools
import math

import jax
import jax.numpy as jnp
from jax import lax
from jax.experimental import pallas as pl
from jax.experimental.pallas import tpu as pltpu
from jax.sharding import PartitionSpec as P

MESH = pl.DeviceIdType.MESH
LOG2E = math.log2(math.e)
CHUNK = 8
STEP = 32
GROUPS = 2


def in_three(x):
    high = x.astype(jnp.bfloat16).astype(jnp.float32)
    middle = (x - high).astype(jnp.bfloat16).astype(jnp.float32)
    return high, middle, x - high - middle


def exchange_kernel(
    own, levels, gases, columns, share, subs,
    gas_hbm, mass_hbm, state_hbm, table_hbm, omega_hbm, weight_hbm,
    gas_out, mass_out, state_out, path_out, pass_out, beam_out, half_out, top_out,
    table_v, omega_v, weight_v, pack_v, lay_v, spread_v, in_sem, send_sem, recv_sem,
):
    band = lax.axis_index("band")
    sub = lax.axis_index("sub")
    gpoints = share * subs
    rows = gpoints // GROUPS
    width = CHUNK * gases
    barrier = pltpu.get_barrier_semaphore()
    for step in range(1, subs):
        pl.semaphore_signal(barrier, inc=1, device_id=(band, lax.rem(sub + step, subs)), device_id_type=MESH)
    tables = ((table_hbm, table_v), (omega_hbm, omega_v), (weight_hbm, weight_v))
    copies = [pltpu.make_async_copy(source, target, in_sem.at[k]) for k, (source, target) in enumerate(tables)]
    blocks = ((gas_hbm, gas_out), (mass_hbm, mass_out), (state_hbm, state_out))
    others = [
        pltpu.make_async_copy(source.at[pl.ds(sub * own, own)], target, in_sem.at[3 + k])
        for k, (source, target) in enumerate(blocks)
    ]
    for copy in copies + others:
        copy.start()
    lay_v[...] = jnp.zeros_like(lay_v)
    spread_v[...] = jnp.zeros_like(spread_v)
    for copy in copies:
        copy.wait()
    pack_v[sub, 0:gases, 0:share] = table_v[...].astype(jnp.float32)
    pack_v[sub, 0:1, 32 : 32 + share] = omega_v[...]
    pack_v[sub, 0:1, 64 : 64 + share] = weight_v[...]
    pl.semaphore_wait(barrier, subs - 1)
    sent = []
    for step in range(1, subs):
        copy = pltpu.make_async_remote_copy(
            src_ref=pack_v.at[sub],
            dst_ref=pack_v.at[sub],
            send_sem=send_sem.at[step],
            recv_sem=recv_sem.at[step],
            device_id=(band, lax.rem(sub + step, subs)),
            device_id_type=MESH,
        )
        copy.start()
        sent.append(copy)
    for copy in others:
        copy.wait()

    slants = [
        jnp.broadcast_to((-LOG2E) / state_out[j].astype(jnp.float32)[0:1, :], (8, columns)) for j in range(own)
    ]

    def add_layers(m, totals):
        at = pl.ds(pl.multiple_of(m * 16, 16), 16)
        after = []
        for j in range(own):
            amounts = gas_out[j, at, :].astype(jnp.float32)
            upper = totals[j] + amounts[:8]
            lower = upper + amounts[8:]
            both = jnp.concatenate([upper * slants[j], lower * slants[j]], axis=0)
            for k, term in enumerate(in_three(both)):
                path_out[k, j, at, :] = term.astype(jnp.bfloat16)
            after.append(lower)
        return tuple(after)

    lax.fori_loop(0, levels // 2, add_layers, tuple(jnp.zeros_like(slant) for slant in slants))
    for copy in sent:
        copy.wait()

    for s in range(subs):
        at = slice(s * share, (s + 1) * share)
        lay_v[0:gases, at] = pack_v[s, 0:gases, 0:share]
        lay_v[gases : gases + 1, at] = pack_v[s, 0:1, 32 : 32 + share]
        lay_v[gases + 1 : gases + 2, at] = pack_v[s, 0:1, 64 : 64 + share]
    by_row = jnp.transpose(lay_v[...])[:gpoints]
    weight = by_row[:, gases + 1 : gases + 2]
    half_out[...] = jnp.broadcast_to(0.5 * by_row[:, gases : gases + 1], (gpoints, columns))
    top_out[...] = jnp.broadcast_to(weight, (gpoints, columns))

    def spread(parts, target):
        for k, part in enumerate(parts):
            for g in range(GROUPS):
                for l in range(CHUNK):
                    at = k * width + l * gases
                    spread_v[pl.ds((g * CHUNK + l) * rows, rows), at : at + gases] = part[g * rows : (g + 1) * rows]
        target[...] = spread_v[:, : target.shape[1]].astype(jnp.bfloat16)

    absorbed = by_row[:, :gases]
    parts = in_three(absorbed * (-LOG2E))
    spread(parts, pass_out)
    lane = lax.broadcasted_iota(jnp.int32, (gpoints, 16), 1)
    logs = jnp.zeros((gpoints, 16), jnp.float32)
    for k, part in enumerate(in_three(jnp.log(weight) * LOG2E)):
        logs = jnp.where(lane == k, jnp.broadcast_to(part, logs.shape), logs)
    for g in range(GROUPS):
        for l in range(CHUNK):
            spread_v[pl.ds((g * CHUNK + l) * rows, rows), 3 * width : 3 * width + 16] = logs[g * rows : (g + 1) * rows]
    spread([absorbed] * 3, beam_out)


def exchange(gas, layer_mass, column_state, absorption, single_scatter, solar_weight, subs):
    share, gases = absorption.shape
    blocks, depth, columns = gas.shape
    own, levels, gpoints = blocks // subs, depth // gases, share * subs
    anywhere = pl.BlockSpec(memory_space=pltpu.HBM)
    vmem = pl.BlockSpec(memory_space=pltpu.VMEM)
    return pl.pallas_call(
        functools.partial(exchange_kernel, own, levels, gases, columns, share, subs),
        out_shape=(
            pltpu.VMEM((own, depth, columns), jnp.bfloat16),
            pltpu.VMEM((own, levels, columns), jnp.bfloat16),
            pltpu.VMEM((own, 2, columns), jnp.bfloat16),
            pltpu.VMEM((3, own, depth, columns), jnp.bfloat16),
            pltpu.VMEM((CHUNK * gpoints, 3 * CHUNK * gases), jnp.bfloat16),
            pltpu.VMEM((CHUNK * gpoints, 3 * CHUNK * gases + 16), jnp.bfloat16),
            pltpu.VMEM((gpoints, columns), jnp.float32),
            pltpu.VMEM((gpoints, columns), jnp.float32),
        ),
        in_specs=[anywhere] * 6,
        out_specs=[vmem] * 8,
        scratch_shapes=[
            pltpu.VMEM((gases, share), jnp.bfloat16),
            pltpu.VMEM((1, share), jnp.float32),
            pltpu.VMEM((1, share), jnp.float32),
            pltpu.VMEM((subs, 8, 128), jnp.float32),
            pltpu.VMEM((16, 128), jnp.float32),
            pltpu.VMEM((CHUNK * gpoints, 3 * CHUNK * gases + 16), jnp.float32),
            pltpu.SemaphoreType.DMA((6,)),
            pltpu.SemaphoreType.DMA((subs,)),
            pltpu.SemaphoreType.DMA((subs,)),
        ],
        compiler_params=pltpu.CompilerParams(
            collective_id=0, has_side_effects=True, vmem_limit_bytes=61500000
        ),
        name="exchange_tables",
    )(gas, layer_mass, column_state, absorption.T, single_scatter.reshape(1, share), solar_weight.reshape(1, share))


def kernel(
    own, levels, gases, columns, gpoints, subs,
    gas_v, mass_v, state_v, path_v, pass_coef, beam_coef, half_v, top_v, sunlit_hbm,
    heat_hbm, surf_hbm,
    sunlit_s, pass_00, pass_01, pass_10, pass_11, beam_00, beam_01, beam_10, beam_11, square_0, square_1, upper_0, upper_1, lower_0, lower_1, net_0, net_v, flux_v, heat_v, surf_v,
    in_sem, out_sem,
):
    band = lax.axis_index("band")
    sub = lax.axis_index("sub")
    rows = gpoints // GROUPS
    tiles = rows // 8
    steps = levels // STEP
    dots = STEP // CHUNK
    width = CHUNK * gases

    lit_copy = pltpu.make_async_copy(sunlit_hbm, sunlit_s, in_sem.at[0])
    lit_copy.start()

    passes = ((pass_00, pass_01), (pass_10, pass_11))
    beams, squares = ((beam_00, beam_01), (beam_10, beam_11)), (square_0, square_1)
    uppers, lowers, nets = (upper_0, upper_1), (lower_0, lower_1), (net_0, net_v)

    def state_row(j, k):
        row = state_v[j].astype(jnp.float32)[k : k + 1, :]
        return jnp.broadcast_to(row, (8, columns))

    def all_rows(row):
        return jnp.broadcast_to(row[None], (tiles, 8, columns)).reshape(rows, columns)

    def optical(j, g, at):
        amounts = jnp.concatenate([gas_v[j, a, :] for a in at], axis=1)
        amounts = jnp.concatenate([amounts] * 3, axis=0)
        return jnp.dot(pass_coef[pl.ds(g * CHUNK * rows, CHUNK * rows), :], amounts, preferred_element_type=jnp.float32)

    def sunbeam(j, g, at):
        path = [jnp.concatenate([path_v[k, j, a, :] for a in at], axis=1) for k in range(3)]
        path = jnp.concatenate(path + [jnp.ones((16, dots * columns), jnp.bfloat16)], axis=0)
        return jnp.dot(beam_coef[pl.ds(g * CHUNK * rows, CHUNK * rows), :], path, preferred_element_type=jnp.float32)

    def prepare(make, targets, j, slot, g, i):
        logs = make(j, g, [pl.ds(pl.multiple_of((i * dots + d) * width, width), width) for d in range(dots)])
        for d in range(dots):
            for m in range(CHUNK):
                part = logs[m * rows : (m + 1) * rows, d * columns : (d + 1) * columns]
                targets[slot][g][i * STEP + d * CHUNK + m] = part

    def run(down, up, coming, late=None):
        start = ()
        if up is not None:
            ground = all_rows(state_row(up[0], 1))
            start += (ground, jnp.ones_like(ground))
        if down is not None:
            top = top_v[pl.ds(down[2] * rows, rows), :]
            start += (top, jnp.zeros_like(top))

        def body(i, carry):
            carry = list(carry)
            if up is not None:
                _, slot, g = up
                upper, lower = carry[:2]
                half_up = half_v[pl.ds(g * rows, rows), :]
            if down is not None:
                _, slot_d, g_d = down
                beam, scaled = carry[-2:]
                half_down = half_v[pl.ds(g_d * rows, rows), :]
            for k in range(STEP):
                if up is not None:
                    l = levels - 1 - (i * STEP + k)
                    passing = jnp.exp2(passes[slot][g][l])
                    squares[g][l] = passing
                    square = passing * passing
                    reflected = half_up - half_up * square
                    lower = 1.0 / (1.0 - reflected * upper)
                    upper = reflected + (square * upper) * lower
                    uppers[g][l] = upper
                    lowers[g][l] = lower
                if down is not None:
                    l = i * STEP + k
                    inverse = lowers[g_d][l]
                    net = (1.0 - uppers[g_d][l]) * (beam + scaled)
                    at = pl.ds(pl.multiple_of(l * 8, 8), 8)
                    net = jnp.sum(net.reshape(tiles, 8, columns), axis=0)
                    nets[g_d][at, :] = net if g_d == 0 else net + nets[0][at, :]
                    beam_next = jnp.exp2(beams[slot_d][g_d][l])
                    scaled = (squares[g_d][l] * scaled + half_down * (beam - beam_next)) * inverse
                    beam = beam_next
            if coming is not None:
                prepare(optical, passes, *coming, i)
                prepare(sunbeam, beams, *coming, i)
            if late is not None:
                prepare(sunbeam, beams, *late, i)
            return (() if up is None else (upper, lower)) + (() if down is None else (beam, scaled))

        end = lax.fori_loop(0, steps, body, start)
        if down is not None:
            beam, diffuse = end[-2:]
            at = pl.ds(levels * 8, 8)
            net = jnp.sum((beam + diffuse).reshape(tiles, 8, columns), axis=0)
            nets[down[2]][at, :] = net if down[2] == 0 else net + nets[0][at, :]

    def heat_copy(j):
        return pltpu.make_async_copy(heat_v.at[j], heat_hbm.at[j], out_sem.at[j])

    def finish(j):
        at = pl.ds(levels * 8, 8)
        bottom = net_v[at, :]
        net_v[at, :] = bottom * (1.0 - state_row(j, 1))
        here = net_v[pl.ds(0, levels, stride=8), :]
        for s in range(1, 8):
            here = here + net_v[pl.ds(s, levels, stride=8), :]
        flux_v[pl.ds(0, levels), :] = here
        flux_v[pl.ds(levels, 1), :] = jnp.sum(net_v[at, :], axis=0, keepdims=True)
        below = flux_v[pl.ds(1, levels), :]
        lit = sunlit_s[(band * subs + sub) * own + j] == 1
        mu = state_row(j, 0)[:1]
        heating = mass_v[j].astype(jnp.float32) * ((here - below) * mu)
        heat_v[j] = jnp.where(lit, heating, jnp.zeros_like(heating))
        heat_copy(j).start()
        surface_down = jnp.sum(bottom, axis=0, keepdims=True) * mu
        surf_v[pl.ds(j, 1), :] = jnp.where(lit, surface_down, jnp.zeros_like(surface_down))

    lax.fori_loop(0, steps, lambda i, c: (prepare(optical, passes, 0, 0, 0, i), c)[1], 0)
    run(None, (0, 0, 0), (0, 0, 1), (0, 0, 0))
    lit_copy.wait()

    def pair(p, carry):
        for slot in range(2):
            j = p * 2 + slot
            other = 1 - slot
            run((j, slot, 0), (j, slot, 1), (j + 1, other, 0))
            run((j, slot, 1), (j + 1, other, 0), (j + 1, other, 1))
            finish(j)
        return carry

    lax.fori_loop(0, own // 2 - 1, pair, 0)
    j = own - 2
    run((j, 0, 0), (j, 0, 1), (j + 1, 1, 0))
    run((j, 0, 1), (j + 1, 1, 0), (j + 1, 1, 1))
    finish(j)
    run((j + 1, 1, 0), (j + 1, 1, 1), (j + 1, 0, 0))
    run((j + 1, 1, 1), None, None)
    finish(j + 1)
    surf_copy = pltpu.make_async_copy(surf_v, surf_hbm, in_sem.at[1])
    surf_copy.start()
    for j in range(own):
        heat_copy(j).wait()
    surf_copy.wait()


def body(gas_amounts, layer_mass, column_state, absorption, single_scatter, solar_weight, sunlit):
    subs = lax.axis_size("sub")
    blocks, levels, gases, columns = gas_amounts.shape
    share = absorption.shape[0]
    own, gpoints = blocks // subs, share * subs
    anywhere = pl.BlockSpec(memory_space=pltpu.HBM)
    per_level = pltpu.VMEM((levels, gpoints // GROUPS, columns), jnp.float32)
    net = pltpu.VMEM(((levels + 1) * 8, columns), jnp.float32)
    return pl.pallas_call(
        functools.partial(kernel, own, levels, gases, columns, gpoints, subs),
        out_shape=(
            jax.ShapeDtypeStruct((own, levels, columns), jnp.float32),
            jax.ShapeDtypeStruct((own, columns), jnp.float32),
        ),
        in_specs=[pl.BlockSpec(memory_space=pltpu.VMEM)] * 8 + [anywhere],
        out_specs=[anywhere] * 2,
        scratch_shapes=[
            pltpu.SMEM((sunlit.shape[0],), jnp.int32),
        ]
        + [per_level] * 14
        + [
            net, net,
            pltpu.VMEM((levels + 8, columns), jnp.float32),
            pltpu.VMEM((own, levels, columns), jnp.float32),
            pltpu.VMEM((own, columns), jnp.float32),
            pltpu.SemaphoreType.DMA((2,)),
            pltpu.SemaphoreType.DMA((own,)),
        ],
        compiler_params=pltpu.CompilerParams(
            vmem_limit_bytes=40 * 1024 * 1024
        ),
        name="solve_blocks",
    )(
        *exchange(
            gas_amounts.reshape(blocks, levels * gases, columns),
            layer_mass,
            column_state,
            absorption,
            single_scatter,
            solar_weight,
            subs,
        ),
        sunlit,
    )


def solution(mesh):
    in_specs = (
        P("band", None, None, None),
        P("band", None, None),
        P("band", None, None),
        P("sub", None),
        P("sub"),
        P("sub"),
        P(),
    )
    out_specs = (P(("band", "sub"), None, None), P(("band", "sub"), None))
    return jax.shard_map(body, mesh=mesh, in_specs=in_specs, out_specs=out_specs, check_vma=False)
```

```python
import functools
import math

import jax
import jax.numpy as jnp
from jax import lax
from jax.experimental import pallas as pl
from jax.experimental.pallas import tpu as pltpu
from jax.sharding import PartitionSpec as P

MESH = pl.DeviceIdType.MESH
LOG2E = math.log2(math.e)
CHUNK = 8
STEP = 32
GROUPS = 2


def in_three(x):
    high = x.astype(jnp.bfloat16).astype(jnp.float32)
    middle = (x - high).astype(jnp.bfloat16).astype(jnp.float32)
    return high, middle, x - high - middle


def exchange_kernel(
    own, levels, gases, columns, share, subs,
    gas_hbm, mass_hbm, state_hbm, table_hbm, omega_hbm, weight_hbm,
    gas_out, mass_out, state_out, path_out, pass_out, beam_out, half_out, top_out,
    table_v, omega_v, weight_v, lay_v, spread_v, in_sem, send_sem, recv_sem,
):
    band = lax.axis_index("band")
    sub = lax.axis_index("sub")
    gpoints = share * subs
    rows = gpoints // GROUPS
    width = CHUNK * gases
    barrier = pltpu.get_barrier_semaphore()
    for step in range(1, subs):
        pl.semaphore_signal(barrier, inc=1, device_id=(band, lax.rem(sub + step, subs)), device_id_type=MESH)
    tables = ((table_hbm, table_v), (omega_hbm, omega_v), (weight_hbm, weight_v))
    copies = [pltpu.make_async_copy(source, target.at[sub], in_sem.at[k]) for k, (source, target) in enumerate(tables)]
    blocks = ((gas_hbm, gas_out), (mass_hbm, mass_out), (state_hbm, state_out))
    others = [
        pltpu.make_async_copy(source.at[pl.ds(sub * own, own)], target, in_sem.at[3 + k])
        for k, (source, target) in enumerate(blocks)
    ]
    for copy in copies + others:
        copy.start()
    lay_v[...] = jnp.zeros_like(lay_v)
    spread_v[...] = jnp.zeros_like(spread_v)
    for copy in copies:
        copy.wait()
    pl.semaphore_wait(barrier, subs - 1)
    sent = []
    for step in range(1, subs):
        for k, (_, held) in enumerate(tables):
            copy = pltpu.make_async_remote_copy(
                src_ref=held.at[sub],
                dst_ref=held.at[sub],
                send_sem=send_sem.at[step, k],
                recv_sem=recv_sem.at[step, k],
                device_id=(band, lax.rem(sub + step, subs)),
                device_id_type=MESH,
            )
            copy.start()
            sent.append(copy)
    for copy in others:
        copy.wait()

    slants = [
        jnp.broadcast_to((-LOG2E) / state_out[j].astype(jnp.float32)[0:1, :], (8, columns)) for j in range(own)
    ]

    def add_layers(m, totals):
        at = pl.ds(pl.multiple_of(m * 16, 16), 16)
        after = []
        for j in range(own):
            amounts = gas_out[j, at, :].astype(jnp.float32)
            upper = totals[j] + amounts[:8]
            lower = upper + amounts[8:]
            both = jnp.concatenate([upper * slants[j], lower * slants[j]], axis=0)
            for k, term in enumerate(in_three(both)):
                path_out[k, j, at, :] = term.astype(jnp.bfloat16)
            after.append(lower)
        return tuple(after)

    lax.fori_loop(0, levels // 2, add_layers, tuple(jnp.zeros_like(slant) for slant in slants))
    for copy in sent:
        copy.wait()

    for s in range(subs):
        at = slice(s * share, (s + 1) * share)
        lay_v[0:gases, at] = table_v[s].astype(jnp.float32)
        lay_v[gases : gases + 1, at] = omega_v[s]
        lay_v[gases + 1 : gases + 2, at] = weight_v[s]
    by_row = jnp.transpose(lay_v[...])[:gpoints]
    weight = by_row[:, gases + 1 : gases + 2]
    half_out[...] = jnp.broadcast_to(0.5 * by_row[:, gases : gases + 1], (gpoints, columns))
    top_out[...] = jnp.broadcast_to(weight, (gpoints, columns))

    def spread(parts, target):
        for k, part in enumerate(parts):
            for g in range(GROUPS):
                for l in range(CHUNK):
                    at = k * width + l * gases
                    spread_v[pl.ds((g * CHUNK + l) * rows, rows), at : at + gases] = part[g * rows : (g + 1) * rows]
        target[...] = spread_v[:, : target.shape[1]].astype(jnp.bfloat16)

    absorbed = by_row[:, :gases]
    parts = in_three(absorbed * (-LOG2E))
    spread(parts, pass_out)
    lane = lax.broadcasted_iota(jnp.int32, (gpoints, 16), 1)
    logs = jnp.zeros((gpoints, 16), jnp.float32)
    for k, part in enumerate(in_three(jnp.log(weight) * LOG2E)):
        logs = jnp.where(lane == k, jnp.broadcast_to(part, logs.shape), logs)
    for g in range(GROUPS):
        for l in range(CHUNK):
            spread_v[pl.ds((g * CHUNK + l) * rows, rows), 3 * width : 3 * width + 16] = logs[g * rows : (g + 1) * rows]
    spread([absorbed] * 3, beam_out)


def exchange(gas, layer_mass, column_state, absorption, single_scatter, solar_weight, subs):
    share, gases = absorption.shape
    blocks, depth, columns = gas.shape
    own, levels, gpoints = blocks // subs, depth // gases, share * subs
    anywhere = pl.BlockSpec(memory_space=pltpu.HBM)
    vmem = pl.BlockSpec(memory_space=pltpu.VMEM)
    return pl.pallas_call(
        functools.partial(exchange_kernel, own, levels, gases, columns, share, subs),
        out_shape=(
            pltpu.VMEM((own, depth, columns), jnp.bfloat16),
            pltpu.VMEM((own, levels, columns), jnp.bfloat16),
            pltpu.VMEM((own, 2, columns), jnp.bfloat16),
            pltpu.VMEM((3, own, depth, columns), jnp.bfloat16),
            pltpu.VMEM((CHUNK * gpoints, 3 * CHUNK * gases), jnp.bfloat16),
            pltpu.VMEM((CHUNK * gpoints, 3 * CHUNK * gases + 16), jnp.bfloat16),
            pltpu.VMEM((gpoints, columns), jnp.float32),
            pltpu.VMEM((gpoints, columns), jnp.float32),
        ),
        in_specs=[anywhere] * 6,
        out_specs=[vmem] * 8,
        scratch_shapes=[
            pltpu.VMEM((subs, gases, share), jnp.bfloat16),
            pltpu.VMEM((subs, 1, share), jnp.float32),
            pltpu.VMEM((subs, 1, share), jnp.float32),
            pltpu.VMEM((16, 128), jnp.float32),
            pltpu.VMEM((CHUNK * gpoints, 3 * CHUNK * gases + 16), jnp.float32),
            pltpu.SemaphoreType.DMA((6,)),
            pltpu.SemaphoreType.DMA((subs, 3)),
            pltpu.SemaphoreType.DMA((subs, 3)),
        ],
        compiler_params=pltpu.CompilerParams(
            collective_id=0, has_side_effects=True, vmem_limit_bytes=61500000
        ),
        name="exchange_tables",
    )(gas, layer_mass, column_state, absorption.T, single_scatter.reshape(1, share), solar_weight.reshape(1, share))


def kernel(
    own, levels, gases, columns, gpoints, subs,
    gas_v, mass_v, state_v, path_v, pass_coef, beam_coef, half_v, top_v, sunlit_hbm,
    heat_hbm, surf_hbm,
    sunlit_s, pass_00, pass_01, pass_10, pass_11, beam_00, beam_01, beam_10, beam_11, square_0, square_1, upper_0, upper_1, lower_0, lower_1, net_0, net_v, flux_v, heat_v, surf_v,
    in_sem, out_sem,
):
    band = lax.axis_index("band")
    sub = lax.axis_index("sub")
    rows = gpoints // GROUPS
    tiles = rows // 8
    steps = levels // STEP
    dots = STEP // CHUNK
    width = CHUNK * gases

    lit_copy = pltpu.make_async_copy(sunlit_hbm, sunlit_s, in_sem.at[0])
    lit_copy.start()

    passes = ((pass_00, pass_01), (pass_10, pass_11))
    beams, squares = ((beam_00, beam_01), (beam_10, beam_11)), (square_0, square_1)
    uppers, lowers, nets = (upper_0, upper_1), (lower_0, lower_1), (net_0, net_v)

    def state_row(j, k):
        row = state_v[j].astype(jnp.float32)[k : k + 1, :]
        return jnp.broadcast_to(row, (8, columns))

    def all_rows(row):
        return jnp.broadcast_to(row[None], (tiles, 8, columns)).reshape(rows, columns)

    def optical(j, g, at):
        amounts = jnp.concatenate([gas_v[j, a, :] for a in at], axis=1)
        amounts = jnp.concatenate([amounts] * 3, axis=0)
        return jnp.dot(pass_coef[pl.ds(g * CHUNK * rows, CHUNK * rows), :], amounts, preferred_element_type=jnp.float32)

    def sunbeam(j, g, at):
        path = [jnp.concatenate([path_v[k, j, a, :] for a in at], axis=1) for k in range(3)]
        path = jnp.concatenate(path + [jnp.ones((16, dots * columns), jnp.bfloat16)], axis=0)
        return jnp.dot(beam_coef[pl.ds(g * CHUNK * rows, CHUNK * rows), :], path, preferred_element_type=jnp.float32)

    def prepare(make, targets, j, slot, g, i):
        logs = make(j, g, [pl.ds(pl.multiple_of((i * dots + d) * width, width), width) for d in range(dots)])
        for d in range(dots):
            for m in range(CHUNK):
                part = logs[m * rows : (m + 1) * rows, d * columns : (d + 1) * columns]
                targets[slot][g][i * STEP + d * CHUNK + m] = part

    def run(down, up, coming, late=None):
        start = ()
        if up is not None:
            ground = all_rows(state_row(up[0], 1))
            start += (ground, jnp.ones_like(ground))
        if down is not None:
            top = top_v[pl.ds(down[2] * rows, rows), :]
            start += (top, jnp.zeros_like(top))

        def body(i, carry):
            carry = list(carry)
            if up is not None:
                _, slot, g = up
                upper, lower = carry[:2]
                half_up = half_v[pl.ds(g * rows, rows), :]
            if down is not None:
                _, slot_d, g_d = down
                beam, scaled = carry[-2:]
                half_down = half_v[pl.ds(g_d * rows, rows), :]
            for k in range(STEP):
                if up is not None:
                    l = levels - 1 - (i * STEP + k)
                    passing = jnp.exp2(passes[slot][g][l])
                    squares[g][l] = passing
                    square = passing * passing
                    reflected = half_up - half_up * square
                    lower = 1.0 / (1.0 - reflected * upper)
                    upper = reflected + (square * upper) * lower
                    uppers[g][l] = upper
                    lowers[g][l] = lower
                if down is not None:
                    l = i * STEP + k
                    inverse = lowers[g_d][l]
                    net = (1.0 - uppers[g_d][l]) * (beam + scaled)
                    at = pl.ds(pl.multiple_of(l * 8, 8), 8)
                    net = jnp.sum(net.reshape(tiles, 8, columns), axis=0)
                    nets[g_d][at, :] = net if g_d == 0 else net + nets[0][at, :]
                    beam_next = jnp.exp2(beams[slot_d][g_d][l])
                    scaled = (squares[g_d][l] * scaled + half_down * (beam - beam_next)) * inverse
                    beam = beam_next
            if coming is not None:
                prepare(optical, passes, *coming, i)
                prepare(sunbeam, beams, *coming, i)
            if late is not None:
                prepare(sunbeam, beams, *late, i)
            return (() if up is None else (upper, lower)) + (() if down is None else (beam, scaled))

        end = lax.fori_loop(0, steps, body, start)
        if down is not None:
            beam, diffuse = end[-2:]
            at = pl.ds(levels * 8, 8)
            net = jnp.sum((beam + diffuse).reshape(tiles, 8, columns), axis=0)
            nets[down[2]][at, :] = net if down[2] == 0 else net + nets[0][at, :]

    def heat_copy(j):
        return pltpu.make_async_copy(heat_v.at[j], heat_hbm.at[j], out_sem.at[j])

    def finish(j):
        at = pl.ds(levels * 8, 8)
        bottom = net_v[at, :]
        net_v[at, :] = bottom * (1.0 - state_row(j, 1))
        here = net_v[pl.ds(0, levels, stride=8), :]
        for s in range(1, 8):
            here = here + net_v[pl.ds(s, levels, stride=8), :]
        flux_v[pl.ds(0, levels), :] = here
        flux_v[pl.ds(levels, 1), :] = jnp.sum(net_v[at, :], axis=0, keepdims=True)
        below = flux_v[pl.ds(1, levels), :]
        lit = sunlit_s[(band * subs + sub) * own + j] == 1
        mu = state_row(j, 0)[:1]
        heating = mass_v[j].astype(jnp.float32) * ((here - below) * mu)
        heat_v[j] = jnp.where(lit, heating, jnp.zeros_like(heating))
        heat_copy(j).start()
        surface_down = jnp.sum(bottom, axis=0, keepdims=True) * mu
        surf_v[pl.ds(j, 1), :] = jnp.where(lit, surface_down, jnp.zeros_like(surface_down))

    lax.fori_loop(0, steps, lambda i, c: (prepare(optical, passes, 0, 0, 0, i), c)[1], 0)
    run(None, (0, 0, 0), (0, 0, 1), (0, 0, 0))
    lit_copy.wait()

    def pair(p, carry):
        for slot in range(2):
            j = p * 2 + slot
            other = 1 - slot
            run((j, slot, 0), (j, slot, 1), (j + 1, other, 0))
            run((j, slot, 1), (j + 1, other, 0), (j + 1, other, 1))
            finish(j)
        return carry

    lax.fori_loop(0, own // 2 - 1, pair, 0)
    j = own - 2
    run((j, 0, 0), (j, 0, 1), (j + 1, 1, 0))
    run((j, 0, 1), (j + 1, 1, 0), (j + 1, 1, 1))
    finish(j)
    run((j + 1, 1, 0), (j + 1, 1, 1), (j + 1, 0, 0))
    run((j + 1, 1, 1), None, None)
    finish(j + 1)
    surf_copy = pltpu.make_async_copy(surf_v, surf_hbm, in_sem.at[1])
    surf_copy.start()
    for j in range(own):
        heat_copy(j).wait()
    surf_copy.wait()


def body(gas_amounts, layer_mass, column_state, absorption, single_scatter, solar_weight, sunlit):
    subs = lax.axis_size("sub")
    blocks, levels, gases, columns = gas_amounts.shape
    share = absorption.shape[0]
    own, gpoints = blocks // subs, share * subs
    anywhere = pl.BlockSpec(memory_space=pltpu.HBM)
    per_level = pltpu.VMEM((levels, gpoints // GROUPS, columns), jnp.float32)
    net = pltpu.VMEM(((levels + 1) * 8, columns), jnp.float32)
    return pl.pallas_call(
        functools.partial(kernel, own, levels, gases, columns, gpoints, subs),
        out_shape=(
            jax.ShapeDtypeStruct((own, levels, columns), jnp.float32),
            jax.ShapeDtypeStruct((own, columns), jnp.float32),
        ),
        in_specs=[pl.BlockSpec(memory_space=pltpu.VMEM)] * 8 + [anywhere],
        out_specs=[anywhere] * 2,
        scratch_shapes=[
            pltpu.SMEM((sunlit.shape[0],), jnp.int32),
        ]
        + [per_level] * 14
        + [
            net, net,
            pltpu.VMEM((levels + 8, columns), jnp.float32),
            pltpu.VMEM((own, levels, columns), jnp.float32),
            pltpu.VMEM((own, columns), jnp.float32),
            pltpu.SemaphoreType.DMA((2,)),
            pltpu.SemaphoreType.DMA((own,)),
        ],
        compiler_params=pltpu.CompilerParams(
            vmem_limit_bytes=40 * 1024 * 1024
        ),
        name="solve_blocks",
    )(
        *exchange(
            gas_amounts.reshape(blocks, levels * gases, columns),
            layer_mass,
            column_state,
            absorption,
            single_scatter,
            solar_weight,
            subs,
        ),
        sunlit,
    )


def solution(mesh):
    in_specs = (
        P("band", None, None, None),
        P("band", None, None),
        P("band", None, None),
        P("sub", None),
        P("sub"),
        P("sub"),
        P(),
    )
    out_specs = (P(("band", "sub"), None, None), P(("band", "sub"), None))
    return jax.shard_map(body, mesh=mesh, in_specs=in_specs, out_specs=out_specs, check_vma=False)
```
